32 devices in a mesh: field: 8 (over z, x), dom: 4 (over y, core).
Axes of the slice: x: 2, y: 2, z: 4, core: 2. Of those that a mesh axis runs over, the one named last changes fastest.
Arguments:
- coefficients: float32 [256, 128], P('dom'), may hold values from -6 to 6
- copies: int32 [256], P('dom'), may hold values from 1 to 4
- owner: int32 [256, 1], P('dom'), may hold values from 0 to 3; in each aligned block of 64 rows (0 to 63, 64 to 127, ...) at most 32 rows name the same one
- snapshots: int32 [8], replicated, may hold values from 0 to 255
- basis: bfloat16 [4194304, 128], P(('field', 'dom')), may hold values from -3 to 3
- observed: float32 [4194304], P(('field', 'dom')), may hold values from -6 to 6
- precision: float32 [4194304], P(('field', 'dom')), may hold values from 1 to 16
Outputs:
- new_coefficients: float32 [4, 4, 32, 128], P('dom')
The draws below stay inside these ranges and needn't reach their ends.
Inputs may be any that keep to these rules, and one draw needn't show every extreme that they name: Among the 64 particles of one index of dom, at most 32 name the same owner, and in every draw some owner is named by exactly 32 particles of some index of dom.
All inputs are finite; a program needn't handle non-finite values.
Results may differ from the reference program's by a relative error of at most 0.00074.
Values sent between devices are 32-bit elements; how exact they have to be, the bound alone decides.
A program may use at most 192 MiB of HBM per device.

```python
import math
import jax
import jax.numpy as jnp
import numpy as np
from jax import lax

PTS = 4194304
R = 128
NP_DEV = 64
SNAP = 8
NPART = 256
CAP = 32
N_DOM = 4


def basis_values(key):
    normals = jax.random.truncated_normal(jax.random.fold_in(key, 11), -4.0, 4.0, (PTS, R), jnp.float32)
    blended = normals + 0.5 * jnp.roll(normals, 1, axis=1) + 0.3 * jnp.roll(normals, 5, axis=1)
    column_group = jax.random.permutation(jax.random.fold_in(key, 13), R) % 4
    row_group = jnp.arange(PTS, dtype=jnp.int32) % 4
    weighting = jnp.where(row_group[:, None] == column_group[None, :], 1.0, 0.4)
    column_scales = jnp.exp(jax.random.uniform(jax.random.fold_in(key, 17), (R,), jnp.float32, -1.0, 1.0))
    column_scales = column_scales / jnp.sqrt(jnp.mean(column_scales * column_scales))
    values = blended * weighting * column_scales[None, :] / math.sqrt(0.33 * R)
    return jnp.clip(values, -3.0, 3.0)


def draw_basis(key, part):
    return basis_values(key).astype(jnp.bfloat16)


def draw_observed(key, part):
    values = basis_values(key)
    truth_vector = 0.7 * jax.random.normal(jax.random.fold_in(key, 19), (R,), jnp.float32)
    noise_part = 0.5 * jax.random.normal(jax.random.fold_in(key, 23), (PTS,), jnp.float32)
    signal = jnp.dot(values, truth_vector, precision=lax.Precision.HIGHEST)
    return jnp.clip(signal + noise_part, -6.0, 6.0)


def with_ends(values, key, low, top_value):
    longest = values.shape.index(max(values.shape))
    spots = []
    for shift in (0, 1):
        where = [jax.random.randint(jax.random.fold_in(key, axis), (), 0, length) for axis, length in enumerate(values.shape)]
        where[longest] = (where[longest] + shift) % values.shape[longest]
        spots.append(tuple(where))
    return values.at[spots[0]].set(low).at[spots[1]].set(top_value)


def level_of(own_key, shape, split, smallest, high):
    def one(dim, parts):
        heights = jax.random.uniform(jax.random.fold_in(jax.random.fold_in(own_key, 6), dim), (parts,), jnp.float32, smallest / len(split), high / len(split))
        return jnp.repeat(jnp.exp(heights), shape[dim] // parts).reshape((-1,) + (1,) * (len(shape) - dim - 1))

    factor_of = one(*split[0])
    for cut in split[1:]:
        factor_of = factor_of * one(*cut)
    return factor_of


def shared_out(own_key, own, number, rows, number_of, top, reach, skew):
    order = jax.random.permutation(own_key, number_of)
    heavy_load, usual = load_shares(number_of, rows * top, reach, skew, True), load_shares(number_of, rows * top, reach, skew, False)
    places = jnp.arange(number_of)

    def named(tallies, turn):
        used = int((tallies > 0).sum())
        fixed = max(1, used // 4)
        moved = fixed + (places - fixed + turn * (used - fixed)) % max(1, number_of - fixed)
        return jnp.zeros((number_of,), jnp.int32).at[order[jnp.where(places < fixed, places, moved)]].set(jnp.asarray(tallies, jnp.int32))

    tallies = jnp.where(number % 4 == 0, named(heavy_load, number // 4), named(usual, number - number // 4 - 1))
    mixed = jax.random.permutation(jax.random.fold_in(own, 3), number_of)
    giver, receiver = mixed[0:number_of // 2 * 2:2], mixed[1:number_of // 2 * 2:2]
    slack = jnp.minimum(tallies[giver] - 1, reach - tallies[receiver]) // 2
    slack = jnp.where((giver == order[0]) | (receiver == order[0]) | (tallies[receiver] == 0), 0, jnp.maximum(slack, 0))
    moved = jax.random.randint(jax.random.fold_in(own, 4), (number_of // 2,), 0, 1 << 20) % (slack + 1)
    tallies = tallies.at[giver].add(-moved).at[receiver].add(moved)
    labels = jnp.searchsorted(jnp.cumsum(tallies), jnp.arange(rows * top), side="right").astype(jnp.int32)
    table = labels.reshape(top, rows).T
    table = table[jax.random.permutation(jax.random.fold_in(own, 1), rows)]
    turn = jax.random.randint(jax.random.fold_in(own, 2), (rows, 1), 0, top)
    return jnp.take_along_axis(table, (jnp.arange(top)[None, :] + turn) % top, axis=1)


def load_shares(amount, total, bound, skew, full):
    portions = [(1 << 20) // math.isqrt(grade ** skew) + 1 for grade in range(1, amount + 1)]
    largest = bound if full else min(bound, max(-(-total // amount), total * portions[0] // sum(portions)))
    least = 1 if total - largest >= amount - 1 else 0
    given, spare = [largest] + [least] * (amount - 1), total - largest - least * (amount - 1)
    while spare > 0:
        movable = [i for i in range(1, amount) if given[i] < largest] or [i for i in range(1, amount) if given[i] < bound]
        mass, left = sum([portions[i] for i in movable]), spare
        for i in movable:
            more = min(bound - given[i], max(1, left * portions[i] // mass), spare)
            given[i] = given[i] + more
            spare = spare - more
    return np.array(given)


def gaussian(rng, dims, scale, bound, split=(), kind=jnp.bfloat16):
    level = level_of(rng, dims, split, -0.22, 0.18) if split else 1.0
    entries = jax.random.normal(rng, dims, jnp.float32) * scale * level
    return jnp.minimum(jnp.maximum(entries, -bound), bound).astype(kind)


def setup_inputs(seed: int = 0) -> dict:
    streams_of = jax.random.split(jax.random.key(seed), 8)
    coefficients = gaussian(streams_of[0], (NPART, R), 1.0, 6.0, ((0, 4),), jnp.float32)
    copies = with_ends(jax.random.randint(streams_of[1], (NPART,), 1, 5), jax.random.fold_in(streams_of[1], 1), 1, 4).astype(jnp.int32)
    owner_keys = jax.random.split(jax.random.fold_in(streams_of[2], 1), NPART // NP_DEV)
    owner_turns = jax.random.permutation(jax.random.fold_in(streams_of[2], 3), NPART // NP_DEV)
    owner = jax.vmap(lambda own, number: shared_out(jax.random.fold_in(streams_of[2], 2), own, number, NP_DEV, N_DOM, 1, CAP, 2))(owner_keys, owner_turns).reshape((NPART, 1))
    snapshots = with_ends(jax.random.randint(streams_of[3], (SNAP,), 0, NPART), jax.random.fold_in(streams_of[3], 1), 0, NPART - 1).astype(jnp.int32)
    basis = draw_basis(jax.random.fold_in(streams_of[7], 71), 0)
    observed = draw_observed(jax.random.fold_in(streams_of[7], 71), 0)
    precision = jnp.clip(jnp.exp(math.log(16.0) - 2.7725887 * jax.random.uniform(streams_of[6], (PTS,), jnp.float32) ** level_of(streams_of[6], (PTS,), ((0, 32),), -0.2, 0.2)), 1.0, 16.0)
    return {"coefficients": coefficients, "copies": copies, "owner": owner, "snapshots": snapshots, "basis": basis, "observed": observed, "precision": precision}


highest = lax.Precision.HIGHEST

def reference(coefficients, copies, owner, snapshots, basis, observed, precision):
    density = R / PTS
    rounded = coefficients.astype(jnp.bfloat16)
    picked = rounded[snapshots]
    block_width = math.gcd(PTS, 16384)
    last_pair = (((1,), (1,)), ((), ()))

    def point_block(sums_carry, block_index):
        grad_sum, hess_sum = sums_carry
        row_start = block_index * block_width
        basis_rows = lax.dynamic_slice_in_dim(basis, row_start, block_width, 0)
        observed_part = lax.dynamic_slice_in_dim(observed, row_start, block_width, 0)
        precision_part = lax.dynamic_slice_in_dim(precision, row_start, block_width, 0)
        field_values = lax.dot_general(rounded.astype(jnp.float32), basis_rows.astype(jnp.float32), last_pair, preferred_element_type=jnp.float32)
        pulled = (density * precision_part * jnp.tanh(field_values - observed_part)).astype(jnp.bfloat16)
        grad_sum = grad_sum + jnp.dot(pulled.astype(jnp.float32), basis_rows.astype(jnp.float32), preferred_element_type=jnp.float32)
        snap_values = lax.dot_general(picked.astype(jnp.float32), basis_rows.astype(jnp.float32), last_pair, preferred_element_type=jnp.float32)
        slopes = jnp.tanh(snap_values - observed_part)
        bending = density * precision_part * (1.0 - slopes * slopes)
        scaled = (bending[:, :, None] * basis_rows.astype(jnp.float32)[None]).astype(jnp.bfloat16)
        hess_sum = hess_sum + jnp.einsum('spr,pq->srq', scaled.astype(jnp.float32), basis_rows.astype(jnp.float32))
        return ((grad_sum, hess_sum), None)
    start_sums = (jnp.zeros((NPART, R), jnp.float32), jnp.zeros((SNAP, R, R), jnp.float32))
    (grad_sum, hess_sum), _ = lax.scan(point_block, start_sums, jnp.arange(PTS // block_width, dtype=jnp.int32))
    hessians = jnp.eye(R, dtype=jnp.float32)[None] + hess_sum
    mean_hess = jnp.mean(hessians, axis=0)
    hess_trace = jnp.trace(mean_hess)
    repulse = 6.0 / hess_trace
    lifted = jnp.dot(coefficients, mean_hess, precision=highest)
    quad_norms = jnp.sum(lifted * coefficients, axis=1)
    cross_terms = lax.dot_general(lifted.astype(jnp.float32), coefficients.astype(jnp.float32), last_pair, precision=highest, preferred_element_type=jnp.float32)
    distance = quad_norms[:, None] + quad_norms[None, :] - 2.0 * cross_terms
    weights = copies.astype(jnp.float32)[None, :] * jnp.exp(-3.0 * distance / hess_trace)
    weight_total = jnp.sum(weights, axis=1)
    weights_low = weights.astype(jnp.bfloat16)
    carried_low = (coefficients + repulse * lifted).astype(jnp.bfloat16)
    numerator = jnp.dot(weights_low.astype(jnp.float32), carried_low.astype(jnp.float32), preferred_element_type=jnp.float32)
    numerator = numerator + jnp.dot(weights_low.astype(jnp.float32), grad_sum, precision=highest)
    drift_rows = -numerator / weight_total[:, None] + repulse * lifted
    snap_coef = coefficients[snapshots]
    snap_cross = lax.dot_general(lifted.astype(jnp.float32), snap_coef.astype(jnp.float32), last_pair, precision=highest, preferred_element_type=jnp.float32)
    snap_dist = quad_norms[:, None] + quad_norms[snapshots][None, :] - 2.0 * snap_cross
    mixture = 1.0 / jnp.square(1.0 + snap_dist / hess_trace)
    mixture = mixture / jnp.sum(mixture, axis=1, keepdims=True)
    local_hess = jnp.einsum('is,srq->irq', mixture, hessians, precision=highest)
    factor = jnp.linalg.cholesky(local_hess)
    halfway = jax.scipy.linalg.solve_triangular(factor, drift_rows[:, :, None], lower=True)
    newton_step = jax.scipy.linalg.solve_triangular(factor, halfway, lower=True, trans=1)
    updated = coefficients + newton_step[:, :, 0]

    def pack_block(block_moved, block_owner):
        onehot = (block_owner[:, None] == jnp.arange(N_DOM, dtype=jnp.int32)[None, :]).astype(jnp.int32)
        before = jnp.sum(onehot * (jnp.cumsum(onehot, axis=0) - 1), axis=1)
        target = block_owner * CAP + before
        placing = (jnp.arange(N_DOM * CAP, dtype=jnp.int32)[:, None] == target[None, :]).astype(jnp.float32)
        return jnp.dot(placing, block_moved, precision=highest).reshape(N_DOM, CAP, R)
    packed = jax.vmap(pack_block)(updated.reshape(N_DOM, NP_DEV, R), owner[:, 0].reshape(N_DOM, NP_DEV))
    return jnp.transpose(packed, (1, 0, 2, 3))
```

```python
import functools
import math

import jax
import jax.numpy as jnp
from jax import lax
from jax.experimental import pallas as pl
from jax.experimental.pallas import tpu as pltpu
from jax.sharding import PartitionSpec as P

highest = lax.Precision.HIGHEST
last_pair = (((1,), (1,)), ((), ()))
MESH = pl.DeviceIdType.MESH
VMEM = pltpu.MemorySpace.VMEM
GROUP = 8


def round_up(value, unit):
    return -(-value // unit) * unit


def gather_kernel(dom_size, msg_ref, out_ref, send_sem, recv_sem, local_sem):
    me = lax.axis_index("dom")
    barrier = pltpu.get_barrier_semaphore()
    for step in range(1, dom_size):
        peer = lax.rem(me + step, dom_size)
        pl.semaphore_signal(barrier, inc=1, device_id={"dom": peer}, device_id_type=MESH)
    own = pltpu.make_async_copy(msg_ref, out_ref.at[me], local_sem)
    own.start()
    pl.semaphore_wait(barrier, dom_size - 1)
    copies = []
    for step in range(1, dom_size):
        peer = lax.rem(me + step, dom_size)
        copy = pltpu.make_async_remote_copy(
            src_ref=msg_ref,
            dst_ref=out_ref.at[me],
            send_sem=send_sem.at[step - 1],
            recv_sem=recv_sem.at[step - 1],
            device_id={"dom": peer},
            device_id_type=MESH,
        )
        copy.start()
        copies.append(copy)
    own.wait()
    for copy in copies:
        copy.wait()


def gather_dom(msg):
    dom_size = lax.axis_size("dom")
    return pl.pallas_call(
        functools.partial(gather_kernel, dom_size),
        out_shape=jax.ShapeDtypeStruct((dom_size,) + msg.shape, msg.dtype),
        in_specs=[pl.BlockSpec(memory_space=VMEM)],
        out_specs=pl.BlockSpec(memory_space=VMEM),
        scratch_shapes=[
            pltpu.SemaphoreType.DMA((dom_size - 1,)),
            pltpu.SemaphoreType.DMA((dom_size - 1,)),
            pltpu.SemaphoreType.DMA,
        ],
        compiler_params=pltpu.CompilerParams(collective_id=0, has_side_effects=True),
    )(msg)


def local_kernel(density, snaps, coef_ref, basis_ref, obs_ref, prec_ref, out_ref, lhs_ref):
    rows = coef_ref.shape[0]
    particles = rows - 16
    rank = basis_ref.shape[1]
    total = particles + snaps * rank

    @pl.when(pl.program_id(0) == 0)
    def _():
        out_ref[...] = jnp.zeros_like(out_ref)

    basis = basis_ref[...]
    observed = obs_ref[...]
    weight = density * prec_ref[...]
    field = lax.dot_general(coef_ref[...], basis, last_pair, preferred_element_type=jnp.float32)
    slopes = jnp.tanh(field - observed)
    lhs_ref[:particles, :] = (weight * slopes[:particles]).astype(jnp.bfloat16)
    tail = slopes[particles:particles + snaps]
    bend = weight * (1.0 - tail * tail)
    turned = basis.T
    for s in range(snaps):
        row = bend[s:s + 1].astype(jnp.bfloat16)
        lhs_ref[particles + s * rank:particles + (s + 1) * rank, :] = row * turned
    out_ref[:total] += jnp.dot(lhs_ref[...], basis, preferred_element_type=jnp.float32)


def local_sums(density, stacked, snaps, basis, observed, precision, tile, padded):
    points, rank = basis.shape
    particles = stacked.shape[0] - 16
    tile = math.gcd(points, tile)
    total = particles + snaps * rank
    return pl.pallas_call(
        functools.partial(local_kernel, density, snaps),
        grid=(points // tile,),
        in_specs=[
            pl.BlockSpec((particles + 16, rank), lambda i: (0, 0)),
            pl.BlockSpec((tile, rank), lambda i: (i, 0)),
            pl.BlockSpec((1, tile), lambda i: (0, i)),
            pl.BlockSpec((1, tile), lambda i: (0, i)),
        ],
        out_specs=pl.BlockSpec((padded, rank), lambda i: (0, 0)),
        out_shape=jax.ShapeDtypeStruct((padded, rank), jnp.float32),
        scratch_shapes=[pltpu.VMEM((total, tile), jnp.bfloat16)],
        compiler_params=pltpu.CompilerParams(
            dimension_semantics=("arbitrary",), vmem_limit_bytes=56 * 1024 * 1024
        ),
    )(stacked, basis, observed.reshape(1, points), precision.reshape(1, points))


def reduce_kernel(half_dom, peers, part_ref, out_ref, pair_ref, held_ref, land_ref,
                  pair_send, pair_recv, give_send, give_recv, back_send, back_recv,
                  pass_send, pass_recv):
    dom = lax.axis_index("dom")
    field = lax.axis_index("field")
    core = lax.rem(dom, 2)
    other = dom + 1 - 2 * core
    me = field * half_dom + dom // 2

    def place(peer):
        return (peer // half_dom, lax.rem(peer, half_dom) * 2 + core)

    barrier = pltpu.get_barrier_semaphore()

    def greet(step, carry):
        pl.semaphore_signal(
            barrier, inc=1, device_id=place(lax.rem(me + step, peers)), device_id_type=MESH
        )
        return carry

    pl.semaphore_signal(barrier, inc=1, device_id=(field, other), device_id_type=MESH)
    lax.fori_loop(1, peers, greet, 0)
    pl.semaphore_wait(barrier, peers)

    def pair_copy(peer):
        return pltpu.make_async_remote_copy(
            src_ref=part_ref.at[1 - core, peer],
            dst_ref=pair_ref.at[peer],
            send_sem=pair_send.at[peer],
            recv_sem=pair_recv.at[peer],
            device_id=(field, other),
            device_id_type=MESH,
        )

    def give_copy(step):
        peer = lax.rem(me + step, peers)
        return pltpu.make_async_remote_copy(
            src_ref=held_ref.at[peer],
            dst_ref=land_ref.at[step],
            send_sem=give_send.at[step],
            recv_sem=give_recv.at[step],
            device_id=place(peer),
            device_id_type=MESH,
        )

    def back_copy(step):
        return pltpu.make_async_remote_copy(
            src_ref=out_ref.at[core, me],
            dst_ref=out_ref.at[core, me],
            send_sem=back_send.at[step],
            recv_sem=back_recv.at[step],
            device_id=place(lax.rem(me + step, peers)),
            device_id_type=MESH,
        )

    def pass_copy(step):
        peer = lax.rem(me + peers - step, peers)
        return pltpu.make_async_remote_copy(
            src_ref=out_ref.at[core, peer],
            dst_ref=out_ref.at[core, peer],
            send_sem=pass_send.at[step],
            recv_sem=pass_recv.at[step],
            device_id=(field, other),
            device_id_type=MESH,
        )

    def start_pair(step, carry):
        pair_copy(lax.rem(me + step, peers)).start()
        return carry

    lax.fori_loop(1, peers + 1, start_pair, 0)

    def combine(step, carry):
        peer = lax.rem(me + step, peers)
        pair_copy(peer).wait_recv()
        held_ref[peer] = part_ref[core, peer] + pair_ref[peer]

        @pl.when(step < peers)
        def _():
            give_copy(step).start()

        return carry

    lax.fori_loop(1, peers + 1, combine, 0)

    def absorb(step, total):
        give_copy(step).wait_recv()
        return total + land_ref[step]

    out_ref[core, me] = lax.fori_loop(1, peers, absorb, held_ref[me])

    def start_back(step, carry):
        back_copy(step).start()
        return carry

    lax.fori_loop(1, peers, start_back, 0)
    pass_copy(0).start()

    def forward(step, carry):
        back_copy(step).wait_recv()
        pass_copy(step).start()
        return carry

    lax.fori_loop(1, peers, forward, 0)

    def drain(step, carry):
        pass_copy(step).wait_recv()
        pass_copy(step).wait_send()
        pair_copy(step).wait_send()
        return carry

    lax.fori_loop(0, peers, drain, 0)

    def drain_sends(step, carry):
        give_copy(step).wait_send()
        back_copy(step).wait_send()
        return carry

    lax.fori_loop(1, peers, drain_sends, 0)


def reduce_all(part):
    half_dom = lax.axis_size("dom") // 2
    peers = lax.axis_size("field") * half_dom
    rank = part.shape[1]
    piece = part.shape[0] // (2 * peers)
    dma = pltpu.SemaphoreType.DMA
    total = pl.pallas_call(
        functools.partial(reduce_kernel, half_dom, peers),
        out_shape=jax.ShapeDtypeStruct((2, peers, piece, rank), part.dtype),
        in_specs=[pl.BlockSpec(memory_space=VMEM)],
        out_specs=pl.BlockSpec(memory_space=VMEM),
        scratch_shapes=[pltpu.VMEM((peers, piece, rank), part.dtype)] * 3 + [dma((peers,))] * 8,
        compiler_params=pltpu.CompilerParams(collective_id=1, has_side_effects=True),
    )(part.reshape(2, peers, piece, rank))
    return total.reshape(part.shape)


def lane_of(row, lane):
    return jnp.broadcast_to(row[:, lane:lane + 1], row.shape)


def newton_kernel(snaps, total_ref, everyone_ref, counts_ref, own_ref, snap_ref, out_ref,
                  grid_ref):
    particles, rank = everyone_ref.shape
    height = own_ref.shape[0]
    f32 = jnp.float32
    dot = functools.partial(jnp.dot, precision=highest, preferred_element_type=f32)
    turned_dot = functools.partial(
        lax.dot_general, dimension_numbers=last_pair, precision=highest, preferred_element_type=f32
    )
    diagonal = (
        lax.broadcasted_iota(jnp.int32, (rank, rank), 0)
        == lax.broadcasted_iota(jnp.int32, (rank, rank), 1)
    )

    def hess(s):
        return total_ref[particles + s * rank:particles + (s + 1) * rank, :]

    mean = hess(0)
    for s in range(1, snaps):
        mean = mean + hess(s)
    mean = mean * (1.0 / snaps) + jnp.where(diagonal, 1.0, 0.0)
    trace = jnp.sum(jnp.sum(jnp.where(diagonal, mean, 0.0), axis=1, keepdims=True), axis=0, keepdims=True)
    repulse = 6.0 / trace
    everyone = everyone_ref[...]
    own = own_ref[...]
    snap = snap_ref[...]
    ones = jnp.ones((8, rank), f32)
    lifted = dot(everyone, mean)
    own_lift = dot(own, mean)
    snap_lift = dot(snap, mean)
    quad_row = turned_dot(ones, lifted * everyone)[:1]
    snap_row = turned_dot(ones, snap_lift * snap)[:1]
    own_quad = jnp.sum(own_lift * own, axis=1, keepdims=True)
    distance = own_quad + quad_row - 2.0 * turned_dot(own_lift, everyone)
    weights = counts_ref[...] * jnp.exp(-3.0 * distance / trace)
    weight_total = jnp.sum(weights, axis=1, keepdims=True)
    weights_low = weights.astype(jnp.bfloat16)
    carried_low = (everyone + repulse * lifted).astype(jnp.bfloat16)
    numerator = jnp.dot(weights_low, carried_low, preferred_element_type=f32)
    numerator = numerator + dot(weights_low.astype(f32), total_ref[:particles, :])
    drift = -numerator / weight_total + repulse * own_lift
    snap_dist = own_quad + snap_row - 2.0 * turned_dot(own_lift, snap)
    shifted = 1.0 + snap_dist / trace
    mixture = 1.0 / (shifted * shifted)
    mixture = mixture / jnp.sum(mixture, axis=1, keepdims=True)

    shares = [jnp.broadcast_to(mixture[:, s:s + 1], (height, rank)) for s in range(snaps)]
    lanes = lax.broadcasted_iota(jnp.int32, (height, rank), 1)

    def blend(block, carry):
        first = pl.multiple_of(block * 8, 8)
        groups = [total_ref[pl.ds(particles + s * rank + first, 8), :] for s in range(snaps)]
        for r in range(8):
            line = jnp.where(lanes == first + r, 1.0, 0.0)
            for s in range(snaps):
                line = line + shares[s] * groups[s][r:r + 1, :]
            grid_ref[first + r] = line
        return carry

    lax.fori_loop(0, rank // 8, blend, 0)

    state = drift
    for first in range(0, rank, GROUP):
        rows = [grid_ref[first + a] for a in range(GROUP)]
        corner = [[lane_of(rows[a], first + c) if c >= a else None for c in range(GROUP)] for a in range(GROUP)]
        inverse, factors = [], {}
        for a in range(GROUP):
            inverse.append(1.0 / corner[a][a])
            for c in range(a + 1, GROUP):
                factors[a, c] = corner[a][c] * inverse[a]
            for c in range(a + 1, GROUP):
                for e in range(c, GROUP):
                    corner[c][e] = corner[c][e] - factors[a, c] * corner[a][e]
        wiped = []
        for a in range(GROUP):
            line = rows[a]
            for c in range(a):
                line = jnp.where(lanes == first + c, 0.0, line) - factors[c, a] * wiped[c]
            wiped.append(jnp.where(lanes == first + a, 1.0, line))
        inside = (lanes >= first) & (lanes < first + GROUP)
        below = [jnp.where(inside & (lanes > first + a), 0.0, wiped[a]) for a in range(GROUP)]
        scaled = [wiped[a] * inverse[a] for a in range(GROUP)]
        for j in range(first + GROUP, rank):
            line = jnp.where(inside, 0.0, grid_ref[j])
            for a in range(GROUP):
                line = line - lane_of(scaled[a], j) * below[a]
            grid_ref[j] = line
        heads = [lane_of(state, first + a) for a in range(GROUP)]
        for a in range(GROUP):
            for c in range(a + 1, GROUP):
                heads[c] = heads[c] - factors[a, c] * heads[a]
        state = jnp.where(inside, 0.0, state)
        for a in range(GROUP):
            state = state - (heads[a] * inverse[a]) * below[a]
    out_ref[...] = own - state


def newton_rows(snaps, total, everyone, counts, own, snap):
    rank = everyone.shape[1]
    height = own.shape[0]
    return pl.pallas_call(
        functools.partial(newton_kernel, snaps),
        out_shape=jax.ShapeDtypeStruct((height, rank), jnp.float32),
        in_specs=[pl.BlockSpec(memory_space=VMEM)] * 5,
        out_specs=pl.BlockSpec(memory_space=VMEM),
        scratch_shapes=[pltpu.VMEM((rank, height, rank), jnp.float32)],
        compiler_params=pltpu.CompilerParams(vmem_limit_bytes=32 * 1024 * 1024),
    )(total, everyone, counts, own, snap)


def place_kernel(field_size, peers, slots, moved_ref, owner_ref, out_ref, all_ref, send_sem, recv_sem):
    dom = lax.axis_index("dom")
    me = dom * field_size + lax.axis_index("field")
    height = moved_ref.shape[0]
    columns = owner_ref.shape[1]
    spread = out_ref.shape[0]
    barrier = pltpu.get_barrier_semaphore()

    def spot(step):
        peer = lax.rem(me + step, peers)
        return (lax.rem(peer, field_size), peer // field_size)

    def greet(step, carry):
        pl.semaphore_signal(barrier, inc=1, device_id=spot(step), device_id_type=MESH)
        return carry

    def copy_to(step):
        return pltpu.make_async_remote_copy(
            src_ref=moved_ref,
            dst_ref=all_ref.at[me],
            send_sem=send_sem.at[step],
            recv_sem=recv_sem.at[step],
            device_id=spot(step),
            device_id_type=MESH,
        )

    def start(step, carry):
        copy_to(step).start()
        return carry

    def finish(step, carry):
        copy_to(step).wait()
        return carry

    lax.fori_loop(1, peers, greet, 0)
    pl.semaphore_wait(barrier, peers - 1)
    lax.fori_loop(1, peers, start, 0)
    all_ref[me] = moved_ref[...]
    mine = owner_ref[...] == dom.astype(jnp.float32)
    group = field_size * height
    row = lax.broadcasted_iota(jnp.int32, (columns, columns), 0)
    col = lax.broadcasted_iota(jnp.int32, (columns, columns), 1)
    earlier = jnp.where((row < col) & (row // group == col // group), 1.0, 0.0).astype(jnp.bfloat16)
    flags = jnp.broadcast_to(jnp.where(mine, 1.0, 0.0), (8, columns)).astype(jnp.bfloat16)
    before = jnp.dot(flags, earlier, preferred_element_type=jnp.float32)[:1]
    base = (lax.broadcasted_iota(jnp.int32, (1, columns), 1) // group * slots).astype(jnp.float32)
    target = jnp.where(mine, base + before, -1.0)
    lines = lax.broadcasted_iota(jnp.int32, (spread, columns), 0).astype(jnp.float32)
    placing = jnp.where(lines == target, 1.0, 0.0)
    lax.fori_loop(1, peers, finish, 0)
    moved = all_ref[...].reshape(columns, all_ref.shape[2])
    out_ref[...] = jnp.dot(placing, moved, precision=highest, preferred_element_type=jnp.float32)


def place_rows(moved, owners, slots):
    field_size, dom_size = lax.axis_size("field"), lax.axis_size("dom")
    peers = field_size * dom_size
    height, rank = moved.shape
    return pl.pallas_call(
        functools.partial(place_kernel, field_size, peers, slots),
        out_shape=jax.ShapeDtypeStruct((dom_size * slots, rank), jnp.float32),
        in_specs=[pl.BlockSpec(memory_space=VMEM)] * 2,
        out_specs=pl.BlockSpec(memory_space=VMEM),
        scratch_shapes=[
            pltpu.VMEM((peers, height, rank), jnp.float32),
            pltpu.SemaphoreType.DMA((peers,)),
            pltpu.SemaphoreType.DMA((peers,)),
        ],
        compiler_params=pltpu.CompilerParams(collective_id=2, has_side_effects=True),
    )(moved, owners)


def body(coefficients, copies, owner, snapshots, basis, observed, precision):
    dom_size, field_size = lax.axis_size("dom"), lax.axis_size("field")
    devices = dom_size * field_size
    block_rows, rank = coefficients.shape
    points = basis.shape[0] * devices
    density = rank / points
    snaps = snapshots.shape[0]
    labels = jnp.stack([copies.astype(jnp.float32), owner[:, 0].astype(jnp.float32)])
    labels = jnp.pad(labels, ((0, 6), (0, rank - block_rows)))
    gathered = gather_dom(jnp.concatenate([coefficients, labels], axis=0))
    everyone = gathered[:, :block_rows].reshape(dom_size * block_rows, rank)
    counts = gathered[:, block_rows, :block_rows].reshape(1, dom_size * block_rows)
    owners = gathered[:, block_rows + 1, :block_rows]
    particles = everyone.shape[0]
    snap_coef = everyone[snapshots]
    spare = jnp.zeros((16 - snaps, rank), jnp.float32)
    stacked = jnp.concatenate([everyone, snap_coef, spare], axis=0).astype(jnp.bfloat16)
    padded = round_up(-(-(particles + snaps * rank) // devices), 8) * devices
    part = local_sums(density, stacked, snaps, basis, observed, precision, 2048, padded)
    total = reduce_all(part)
    row_count = block_rows // field_size
    height = round_up(row_count, 8)
    own = lax.dynamic_slice_in_dim(coefficients, lax.axis_index("field") * row_count, row_count, 0)
    own = jnp.pad(own, ((0, height - row_count), (0, 0)))
    moved = newton_rows(snaps, total, everyone, counts, own, snap_coef)
    owner_row = jnp.pad(
        owners.reshape(devices, row_count), ((0, 0), (0, height - row_count)), constant_values=-1.0
    ).reshape(1, devices * height)
    slots = 2 * block_rows // dom_size
    placed = place_rows(moved, owner_row, slots)
    return placed.reshape(1, dom_size, slots, rank)


def solution(mesh):
    return jax.shard_map(
        body,
        mesh=mesh,
        in_specs=(
            P("dom", None),
            P("dom"),
            P("dom", None),
            P(),
            P(("field", "dom"), None),
            P(("field", "dom")),
            P(("field", "dom")),
        ),
        out_specs=P("dom", None, None, None),
        check_vma=False,
    )
```

```python
import functools
import math

import jax
import jax.numpy as jnp
from jax import lax
from jax.experimental import pallas as pl
from jax.experimental.pallas import tpu as pltpu
from jax.sharding import PartitionSpec as P

highest = lax.Precision.HIGHEST
last_pair = (((1,), (1,)), ((), ()))
MESH = pl.DeviceIdType.MESH
VMEM = pltpu.MemorySpace.VMEM
GROUP = 8
TILE, RING = 8192, 8


def round_up(value, unit):
    return -(-value // unit) * unit


def gather_kernel(dom_size, msg_ref, out_ref, send_sem, recv_sem, local_sem):
    me = lax.axis_index("dom")
    barrier = pltpu.get_barrier_semaphore()
    for step in range(1, dom_size):
        peer = lax.rem(me + step, dom_size)
        pl.semaphore_signal(barrier, inc=1, device_id={"dom": peer}, device_id_type=MESH)
    own = pltpu.make_async_copy(msg_ref, out_ref.at[me], local_sem)
    own.start()
    pl.semaphore_wait(barrier, dom_size - 1)
    copies = []
    for step in range(1, dom_size):
        peer = lax.rem(me + step, dom_size)
        copy = pltpu.make_async_remote_copy(
            src_ref=msg_ref,
            dst_ref=out_ref.at[me],
            send_sem=send_sem.at[step - 1],
            recv_sem=recv_sem.at[step - 1],
            device_id={"dom": peer},
            device_id_type=MESH,
        )
        copy.start()
        copies.append(copy)
    own.wait()
    for copy in copies:
        copy.wait()


def gather_dom(msg):
    dom_size = lax.axis_size("dom")
    return pl.pallas_call(
        functools.partial(gather_kernel, dom_size),
        out_shape=jax.ShapeDtypeStruct((dom_size,) + msg.shape, msg.dtype),
        in_specs=[pl.BlockSpec(memory_space=VMEM)],
        out_specs=pl.BlockSpec(memory_space=VMEM),
        scratch_shapes=[
            pltpu.SemaphoreType.DMA((dom_size - 1,)),
            pltpu.SemaphoreType.DMA((dom_size - 1,)),
            pltpu.SemaphoreType.DMA,
        ],
        compiler_params=pltpu.CompilerParams(collective_id=0, has_side_effects=True),
    )(msg)


def local_kernel(density, snaps, coef_ref, basis_ref, obs_ref, prec_ref, out_ref, lhs_ref):
    rows = coef_ref.shape[0]
    particles = rows - 16
    rank = basis_ref.shape[1]
    total = particles + snaps * rank

    @pl.when(pl.program_id(0) == 0)
    def _():
        out_ref[...] = jnp.zeros_like(out_ref)

    basis = basis_ref[...]
    observed = obs_ref[...]
    weight = density * prec_ref[...]
    field = lax.dot_general(coef_ref[...], basis, last_pair, preferred_element_type=jnp.float32)
    slopes = jnp.tanh(field - observed)
    lhs_ref[:particles, :] = (weight * slopes[:particles]).astype(jnp.bfloat16)
    tail = slopes[particles:particles + snaps]
    bend = weight * (1.0 - tail * tail)
    turned = basis.T
    for s in range(snaps):
        row = bend[s:s + 1].astype(jnp.bfloat16)
        lhs_ref[particles + s * rank:particles + (s + 1) * rank, :] = row * turned
    out_ref[:total] += jnp.dot(lhs_ref[...], basis, preferred_element_type=jnp.float32)


def local_sums(density, stacked, snaps, basis, observed, precision, tile, padded):
    points, rank = basis.shape
    particles = stacked.shape[0] - 16
    tile = math.gcd(points, tile)
    total = particles + snaps * rank
    return pl.pallas_call(
        functools.partial(local_kernel, density, snaps),
        grid=(points // tile,),
        in_specs=[
            pl.BlockSpec((particles + 16, rank), lambda i: (0, 0)),
            pl.BlockSpec((tile, rank), lambda i: (i, 0)),
            pl.BlockSpec((1, tile), lambda i: (0, i)),
            pl.BlockSpec((1, tile), lambda i: (0, i)),
        ],
        out_specs=pl.BlockSpec((padded, rank), lambda i: (0, 0)),
        out_shape=jax.ShapeDtypeStruct((padded, rank), jnp.float32),
        scratch_shapes=[pltpu.VMEM((total, tile), jnp.bfloat16)],
        compiler_params=pltpu.CompilerParams(
            dimension_semantics=("arbitrary",), vmem_limit_bytes=56 * 1024 * 1024
        ),
    )(stacked, basis, observed.reshape(1, points), precision.reshape(1, points))


CHUNK = 256
PIECE = 64


def held_kernel(density, snaps, ring, coef_ref, basis_ref, obs_ref, prec_ref, out_ref, lhs_ref, wide_ref, side_ref):
    tile, rank = basis_ref.shape
    particles = coef_ref.shape[0] - 16
    pieces = particles // PIECE
    split = particles + snaps // 2 * rank
    chunks = tile // CHUNK
    f32 = jnp.float32
    push, multiply, pop = pltpu.matmul_push_rhs, pltpu.matmul_acc_lhs, pltpu.matmul_pop

    def run(tails, fields, first_a, second_a, first_b, second_b):
        @pl.when(pl.program_id(0) == 0)
        def _():
            out_ref[...] = jnp.zeros_like(out_ref)
            side_ref[...] = jnp.zeros_like(side_ref)
            wide_ref[...] = jnp.zeros_like(wide_ref)
            for ref in [*tails, *fields, first_a, second_a, first_b, second_b]:
                pop(ref)

        def slot(c):
            return slice(c % ring * CHUNK, (c % ring + 1) * CHUNK)

        def prepare(c):
            points, held, turn = slice(c * CHUNK, (c + 1) * CHUNK), slot(c), c % 2
            basis = basis_ref[points, :]
            wide_ref[held, :rank] = basis
            push(wide_ref[held, :], staging_register=turn, mxu_index=0, transpose=True)
            turned = basis.T
            multiply(tails[turn], coef_ref[particles:, :], load_staged_rhs=turn)
            for q in range(pieces):
                multiply(fields[turn * pieces + q], coef_ref[q * PIECE:(q + 1) * PIECE, :])
            observed = obs_ref[:, points]
            weight = density * prec_ref[:, points]
            slopes = jnp.tanh(pop(tails[turn])[:snaps] - observed)
            bend = weight * (1.0 - slopes * slopes)
            for s in range(snaps):
                start = particles + s * rank
                lhs_ref[start:start + rank, held] = bend[s:s + 1].astype(jnp.bfloat16) * turned
            for q in range(pieces):
                slopes = jnp.tanh(pop(fields[turn * pieces + q]) - observed)
                lhs_ref[q * PIECE:(q + 1) * PIECE, held] = (weight * slopes).astype(jnp.bfloat16)
            return turned

        def consume(c, turned):
            held = slot(c)
            one = c % 2
            two = 1 - one
            wide = wide_ref[held, :]
            if c + 1 >= chunks:
                one, two = two, one
            push(wide, staging_register=one, mxu_index=0)
            push(wide, staging_register=0, mxu_index=1)
            multiply(first_a, lhs_ref[:particles, held], load_staged_rhs=one)
            multiply(second_a, lhs_ref[particles:split, held], load_staged_rhs=0)
            push(lhs_ref[split:split + CHUNK, held], staging_register=two, mxu_index=0, transpose=True)
            push(lhs_ref[split + CHUNK:, held], staging_register=1, mxu_index=1, transpose=True)
            multiply(first_b, turned, load_staged_rhs=two)
            multiply(second_b, turned, load_staged_rhs=1)

        turned = prepare(0)
        for c in range(chunks):
            after = prepare(c + 1) if c + 1 < chunks else None
            consume(c, turned)
            turned = after
        out_ref[:particles, :] += pop(first_a)[:, :rank]
        out_ref[particles:split, :] += pop(second_a)[:, :rank]
        side_ref[:, :CHUNK] += pop(first_b)
        side_ref[:, CHUNK:] += pop(second_b)

        @pl.when(pl.program_id(0) == pl.num_programs(0) - 1)
        def _():
            for t in range(2 * CHUNK // rank):
                start = split + t * rank
                out_ref[start:start + rank, :] = side_ref[:, t * rank:(t + 1) * rank].T

    unit0, unit1 = pltpu.ACC(0), pltpu.ACC(1)
    pl.run_scoped(
        run,
        [unit0((16, CHUNK), f32)] * 2,
        [unit0((PIECE, CHUNK), f32)] * (2 * pieces),
        unit0((particles, CHUNK), f32),
        unit1((split - particles, CHUNK), f32),
        unit0((rank, CHUNK), f32),
        unit1((rank, CHUNK), f32),
    )


def held_fits(particles, snaps, rank, points):
    entries0 = 2 * (particles + 16) + particles + rank
    entries1 = snaps // 2 * rank + rank
    return (
        2 * rank == CHUNK
        and snaps * rank == 4 * CHUNK
        and particles % PIECE == 0
        and max(entries0, entries1) <= 1024
        and points % CHUNK == 0
    )


def held_sums(density, stacked, snaps, basis, observed, precision, tile, ring, padded):
    points, rank = basis.shape
    particles = stacked.shape[0] - 16
    tile = math.gcd(points, tile)
    total = particles + snaps * rank
    stacked = jnp.concatenate([stacked, jnp.zeros_like(stacked)], axis=1)
    return pl.pallas_call(
        functools.partial(held_kernel, density, snaps, ring),
        grid=(points // tile,),
        in_specs=[
            pl.BlockSpec((particles + 16, 2 * rank), lambda i: (0, 0)),
            pl.BlockSpec((tile, rank), lambda i: (i, 0)),
            pl.BlockSpec((1, tile), lambda i: (0, i)),
            pl.BlockSpec((1, tile), lambda i: (0, i)),
        ],
        out_specs=pl.BlockSpec((padded, rank), lambda i: (0, 0)),
        out_shape=jax.ShapeDtypeStruct((padded, rank), jnp.float32),
        scratch_shapes=[
            pltpu.VMEM((total, ring * CHUNK), jnp.bfloat16),
            pltpu.VMEM((ring * CHUNK, 2 * rank), jnp.bfloat16),
            pltpu.VMEM((rank, 2 * CHUNK), jnp.float32),
        ],
        compiler_params=pltpu.CompilerParams(
            dimension_semantics=("arbitrary",), vmem_limit_bytes=56 * 1024 * 1024
        ),
    )(stacked, basis, observed.reshape(1, points), precision.reshape(1, points))


def reduce_kernel(half_dom, peers, part_ref, out_ref, pair_ref, held_ref, land_ref,
                  pair_send, pair_recv, give_send, give_recv, back_send, back_recv,
                  pass_send, pass_recv):
    dom = lax.axis_index("dom")
    field = lax.axis_index("field")
    core = lax.rem(dom, 2)
    other = dom + 1 - 2 * core
    me = field * half_dom + dom // 2

    def place(peer):
        return (peer // half_dom, lax.rem(peer, half_dom) * 2 + core)

    barrier = pltpu.get_barrier_semaphore()

    def greet(step, carry):
        pl.semaphore_signal(
            barrier, inc=1, device_id=place(lax.rem(me + step, peers)), device_id_type=MESH
        )
        return carry

    pl.semaphore_signal(barrier, inc=1, device_id=(field, other), device_id_type=MESH)
    lax.fori_loop(1, peers, greet, 0)
    pl.semaphore_wait(barrier, peers)

    def pair_copy(peer):
        return pltpu.make_async_remote_copy(
            src_ref=part_ref.at[1 - core, peer],
            dst_ref=pair_ref.at[peer],
            send_sem=pair_send.at[peer],
            recv_sem=pair_recv.at[peer],
            device_id=(field, other),
            device_id_type=MESH,
        )

    def give_copy(step):
        peer = lax.rem(me + step, peers)
        return pltpu.make_async_remote_copy(
            src_ref=held_ref.at[peer],
            dst_ref=land_ref.at[step],
            send_sem=give_send.at[step],
            recv_sem=give_recv.at[step],
            device_id=place(peer),
            device_id_type=MESH,
        )

    def back_copy(step):
        return pltpu.make_async_remote_copy(
            src_ref=out_ref.at[core, me],
            dst_ref=out_ref.at[core, me],
            send_sem=back_send.at[step],
            recv_sem=back_recv.at[step],
            device_id=place(lax.rem(me + step, peers)),
            device_id_type=MESH,
        )

    def pass_copy(step):
        peer = lax.rem(me + peers - step, peers)
        return pltpu.make_async_remote_copy(
            src_ref=out_ref.at[core, peer],
            dst_ref=out_ref.at[core, peer],
            send_sem=pass_send.at[step],
            recv_sem=pass_recv.at[step],
            device_id=(field, other),
            device_id_type=MESH,
        )

    def start_pair(step, carry):
        pair_copy(lax.rem(me + step, peers)).start()
        return carry

    lax.fori_loop(1, peers + 1, start_pair, 0)

    def combine(step, carry):
        peer = lax.rem(me + step, peers)
        pair_copy(peer).wait_recv()
        held_ref[peer] = part_ref[core, peer] + pair_ref[peer]

        @pl.when(step < peers)
        def _():
            give_copy(step).start()

        return carry

    lax.fori_loop(1, peers + 1, combine, 0)

    def absorb(step, total):
        give_copy(step).wait_recv()
        return total + land_ref[step]

    out_ref[core, me] = lax.fori_loop(1, peers, absorb, held_ref[me])

    def start_back(step, carry):
        back_copy(step).start()
        return carry

    lax.fori_loop(1, peers, start_back, 0)
    pass_copy(0).start()

    def forward(step, carry):
        back_copy(step).wait_recv()
        pass_copy(step).start()
        return carry

    lax.fori_loop(1, peers, forward, 0)

    def drain(step, carry):
        pass_copy(step).wait_recv()
        pass_copy(step).wait_send()
        pair_copy(step).wait_send()
        return carry

    lax.fori_loop(0, peers, drain, 0)

    def drain_sends(step, carry):
        give_copy(step).wait_send()
        back_copy(step).wait_send()
        return carry

    lax.fori_loop(1, peers, drain_sends, 0)


def reduce_all(part):
    half_dom = lax.axis_size("dom") // 2
    peers = lax.axis_size("field") * half_dom
    rank = part.shape[1]
    piece = part.shape[0] // (2 * peers)
    dma = pltpu.SemaphoreType.DMA
    total = pl.pallas_call(
        functools.partial(reduce_kernel, half_dom, peers),
        out_shape=jax.ShapeDtypeStruct((2, peers, piece, rank), part.dtype),
        in_specs=[pl.BlockSpec(memory_space=VMEM)],
        out_specs=pl.BlockSpec(memory_space=VMEM),
        scratch_shapes=[pltpu.VMEM((peers, piece, rank), part.dtype)] * 3 + [dma((peers,))] * 8,
        compiler_params=pltpu.CompilerParams(collective_id=1, has_side_effects=True),
    )(part.reshape(2, peers, piece, rank))
    return total.reshape(part.shape)


def lane_of(row, lane):
    return jnp.broadcast_to(row[:, lane:lane + 1], row.shape)


def newton_kernel(snaps, total_ref, everyone_ref, counts_ref, own_ref, snap_ref, out_ref,
                  grid_ref):
    particles, rank = everyone_ref.shape
    height = own_ref.shape[0]
    f32 = jnp.float32
    dot = functools.partial(jnp.dot, precision=highest, preferred_element_type=f32)
    turned_dot = functools.partial(
        lax.dot_general, dimension_numbers=last_pair, precision=highest, preferred_element_type=f32
    )
    diagonal = (
        lax.broadcasted_iota(jnp.int32, (rank, rank), 0)
        == lax.broadcasted_iota(jnp.int32, (rank, rank), 1)
    )

    def hess(s):
        return total_ref[particles + s * rank:particles + (s + 1) * rank, :]

    mean = hess(0)
    for s in range(1, snaps):
        mean = mean + hess(s)
    mean = mean * (1.0 / snaps) + jnp.where(diagonal, 1.0, 0.0)
    trace = jnp.sum(jnp.sum(jnp.where(diagonal, mean, 0.0), axis=1, keepdims=True), axis=0, keepdims=True)
    repulse = 6.0 / trace
    everyone = everyone_ref[...]
    own = own_ref[...]
    snap = snap_ref[...]
    ones = jnp.ones((8, rank), f32)
    lifted = dot(everyone, mean)
    own_lift = dot(own, mean)
    snap_lift = dot(snap, mean)
    quad_row = turned_dot(ones, lifted * everyone)[:1]
    snap_row = turned_dot(ones, snap_lift * snap)[:1]
    own_quad = jnp.sum(own_lift * own, axis=1, keepdims=True)
    distance = own_quad + quad_row - 2.0 * turned_dot(own_lift, everyone)
    weights = counts_ref[...] * jnp.exp(-3.0 * distance / trace)
    weight_total = jnp.sum(weights, axis=1, keepdims=True)
    weights_low = weights.astype(jnp.bfloat16)
    carried_low = (everyone + repulse * lifted).astype(jnp.bfloat16)
    numerator = jnp.dot(weights_low, carried_low, preferred_element_type=f32)
    numerator = numerator + dot(weights_low.astype(f32), total_ref[:particles, :])
    drift = -numerator / weight_total + repulse * own_lift
    snap_dist = own_quad + snap_row - 2.0 * turned_dot(own_lift, snap)
    shifted = 1.0 + snap_dist / trace
    mixture = 1.0 / (shifted * shifted)
    mixture = mixture / jnp.sum(mixture, axis=1, keepdims=True)

    shares = [jnp.broadcast_to(mixture[:, s:s + 1], (height, rank)) for s in range(snaps)]
    lanes = lax.broadcasted_iota(jnp.int32, (height, rank), 1)

    def blend(block, carry):
        first = pl.multiple_of(block * 8, 8)
        groups = [total_ref[pl.ds(particles + s * rank + first, 8), :] for s in range(snaps)]
        for r in range(8):
            line = jnp.where(lanes == first + r, 1.0, 0.0)
            for s in range(snaps):
                line = line + shares[s] * groups[s][r:r + 1, :]
            grid_ref[first + r] = line
        return carry

    lax.fori_loop(0, rank // 8, blend, 0)

    state = drift
    for first in range(0, rank, GROUP):
        rows = [grid_ref[first + a] for a in range(GROUP)]
        corner = [[lane_of(rows[a], first + c) if c >= a else None for c in range(GROUP)] for a in range(GROUP)]
        inverse, factors = [], {}
        for a in range(GROUP):
            inverse.append(1.0 / corner[a][a])
            for c in range(a + 1, GROUP):
                factors[a, c] = corner[a][c] * inverse[a]
            for c in range(a + 1, GROUP):
                for e in range(c, GROUP):
                    corner[c][e] = corner[c][e] - factors[a, c] * corner[a][e]
        wiped = []
        for a in range(GROUP):
            line = rows[a]
            for c in range(a):
                line = jnp.where(lanes == first + c, 0.0, line) - factors[c, a] * wiped[c]
            wiped.append(jnp.where(lanes == first + a, 1.0, line))
        inside = (lanes >= first) & (lanes < first + GROUP)
        below = [jnp.where(inside & (lanes > first + a), 0.0, wiped[a]) for a in range(GROUP)]
        scaled = [wiped[a] * inverse[a] for a in range(GROUP)]
        for j in range(first + GROUP, rank):
            line = jnp.where(inside, 0.0, grid_ref[j])
            for a in range(GROUP):
                line = line - lane_of(scaled[a], j) * below[a]
            grid_ref[j] = line
        heads = [lane_of(state, first + a) for a in range(GROUP)]
        for a in range(GROUP):
            for c in range(a + 1, GROUP):
                heads[c] = heads[c] - factors[a, c] * heads[a]
        state = jnp.where(inside, 0.0, state)
        for a in range(GROUP):
            state = state - (heads[a] * inverse[a]) * below[a]
    out_ref[...] = own - state


def newton_rows(snaps, total, everyone, counts, own, snap):
    rank = everyone.shape[1]
    height = own.shape[0]
    return pl.pallas_call(
        functools.partial(newton_kernel, snaps),
        out_shape=jax.ShapeDtypeStruct((height, rank), jnp.float32),
        in_specs=[pl.BlockSpec(memory_space=VMEM)] * 5,
        out_specs=pl.BlockSpec(memory_space=VMEM),
        scratch_shapes=[pltpu.VMEM((rank, height, rank), jnp.float32)],
        compiler_params=pltpu.CompilerParams(vmem_limit_bytes=32 * 1024 * 1024),
    )(total, everyone, counts, own, snap)


def place_kernel(field_size, peers, slots, moved_ref, owner_ref, out_ref, all_ref, send_sem, recv_sem):
    dom = lax.axis_index("dom")
    me = dom * field_size + lax.axis_index("field")
    height = moved_ref.shape[0]
    columns = owner_ref.shape[1]
    spread = out_ref.shape[0]
    barrier = pltpu.get_barrier_semaphore()

    def spot(step):
        peer = lax.rem(me + step, peers)
        return (lax.rem(peer, field_size), peer // field_size)

    def greet(step, carry):
        pl.semaphore_signal(barrier, inc=1, device_id=spot(step), device_id_type=MESH)
        return carry

    def copy_to(step):
        return pltpu.make_async_remote_copy(
            src_ref=moved_ref,
            dst_ref=all_ref.at[me],
            send_sem=send_sem.at[step],
            recv_sem=recv_sem.at[step],
            device_id=spot(step),
            device_id_type=MESH,
        )

    def start(step, carry):
        copy_to(step).start()
        return carry

    def finish(step, carry):
        copy_to(step).wait()
        return carry

    lax.fori_loop(1, peers, greet, 0)
    pl.semaphore_wait(barrier, peers - 1)
    lax.fori_loop(1, peers, start, 0)
    all_ref[me] = moved_ref[...]
    mine = owner_ref[...] == dom.astype(jnp.float32)
    group = field_size * height
    row = lax.broadcasted_iota(jnp.int32, (columns, columns), 0)
    col = lax.broadcasted_iota(jnp.int32, (columns, columns), 1)
    earlier = jnp.where((row < col) & (row // group == col // group), 1.0, 0.0).astype(jnp.bfloat16)
    flags = jnp.broadcast_to(jnp.where(mine, 1.0, 0.0), (8, columns)).astype(jnp.bfloat16)
    before = jnp.dot(flags, earlier, preferred_element_type=jnp.float32)[:1]
    base = (lax.broadcasted_iota(jnp.int32, (1, columns), 1) // group * slots).astype(jnp.float32)
    target = jnp.where(mine, base + before, -1.0)
    lines = lax.broadcasted_iota(jnp.int32, (spread, columns), 0).astype(jnp.float32)
    placing = jnp.where(lines == target, 1.0, 0.0)
    lax.fori_loop(1, peers, finish, 0)
    moved = all_ref[...].reshape(columns, all_ref.shape[2])
    out_ref[...] = jnp.dot(placing, moved, precision=highest, preferred_element_type=jnp.float32)


def place_rows(moved, owners, slots):
    field_size, dom_size = lax.axis_size("field"), lax.axis_size("dom")
    peers = field_size * dom_size
    height, rank = moved.shape
    return pl.pallas_call(
        functools.partial(place_kernel, field_size, peers, slots),
        out_shape=jax.ShapeDtypeStruct((dom_size * slots, rank), jnp.float32),
        in_specs=[pl.BlockSpec(memory_space=VMEM)] * 2,
        out_specs=pl.BlockSpec(memory_space=VMEM),
        scratch_shapes=[
            pltpu.VMEM((peers, height, rank), jnp.float32),
            pltpu.SemaphoreType.DMA((peers,)),
            pltpu.SemaphoreType.DMA((peers,)),
        ],
        compiler_params=pltpu.CompilerParams(collective_id=2, has_side_effects=True),
    )(moved, owners)


def body(coefficients, copies, owner, snapshots, basis, observed, precision):
    dom_size, field_size = lax.axis_size("dom"), lax.axis_size("field")
    devices = dom_size * field_size
    block_rows, rank = coefficients.shape
    points = basis.shape[0] * devices
    density = rank / points
    snaps = snapshots.shape[0]
    labels = jnp.stack([copies.astype(jnp.float32), owner[:, 0].astype(jnp.float32)])
    labels = jnp.pad(labels, ((0, 6), (0, rank - block_rows)))
    gathered = gather_dom(jnp.concatenate([coefficients, labels], axis=0))
    everyone = gathered[:, :block_rows].reshape(dom_size * block_rows, rank)
    counts = gathered[:, block_rows, :block_rows].reshape(1, dom_size * block_rows)
    owners = gathered[:, block_rows + 1, :block_rows]
    particles = everyone.shape[0]
    snap_coef = everyone[snapshots]
    spare = jnp.zeros((16 - snaps, rank), jnp.float32)
    stacked = jnp.concatenate([everyone, snap_coef, spare], axis=0).astype(jnp.bfloat16)
    padded = round_up(-(-(particles + snaps * rank) // devices), 8) * devices
    if held_fits(particles, snaps, rank, basis.shape[0]):
        part = held_sums(density, stacked, snaps, basis, observed, precision, TILE, RING, padded)
    else:
        part = local_sums(density, stacked, snaps, basis, observed, precision, 4096, padded)
    total = reduce_all(part)
    row_count = block_rows // field_size
    height = round_up(row_count, 8)
    own = lax.dynamic_slice_in_dim(coefficients, lax.axis_index("field") * row_count, row_count, 0)
    own = jnp.pad(own, ((0, height - row_count), (0, 0)))
    moved = newton_rows(snaps, total, everyone, counts, own, snap_coef)
    owner_row = jnp.pad(
        owners.reshape(devices, row_count), ((0, 0), (0, height - row_count)), constant_values=-1.0
    ).reshape(1, devices * height)
    slots = 2 * block_rows // dom_size
    placed = place_rows(moved, owner_row, slots)
    return placed.reshape(1, dom_size, slots, rank)


def solution(mesh):
    return jax.shard_map(
        body,
        mesh=mesh,
        in_specs=(
            P("dom", None),
            P("dom"),
            P("dom", None),
            P(),
            P(("field", "dom"), None),
            P(("field", "dom")),
            P(("field", "dom")),
        ),
        out_specs=P("dom", None, None, None),
        check_vma=False,
    )
```
